256 devices in a mesh: ep: 64 (over z, x, core), tp: 4 (over y).
Axes of the slice: x: 4, y: 4, z: 8, core: 2. Of those that a mesh axis runs over, the one named last changes fastest.
Arguments:
- tokens: bfloat16 [16384, 2048], P('ep', 'tp'), may hold values from -180 to 180
- norm_gain: float32 [2048], replicated, may hold values from 0.1 to 1.9
- router_weight: bfloat16 [2048, 60], P('tp'), may hold values from -2 to 2
- shared_gate_w: bfloat16 [2048], replicated, may hold values from -0.125 to 0.125
- expert_ids: int32 [16384, 4], P('ep'), may hold values from 0 to 59, all different within a row; in each aligned block of 256 rows (0 to 255, 256 to 511, ...) at most 32 rows name the same one
- w_gate: bfloat16 [64, 2048, 1408], P('ep', None, 'tp'), may hold values from -0.125 to 0.125
- w_up: bfloat16 [64, 2048, 1408], P('ep', None, 'tp'), may hold values from -0.125 to 0.125
- w_down: bfloat16 [64, 1408, 2048], P('ep', 'tp'), may hold values from -1.5 to 1.5
- shared_w_gate: bfloat16 [2048, 2816], P(None, 'tp'), may hold values from -0.125 to 0.125
- shared_w_up: bfloat16 [2048, 2816], P(None, 'tp'), may hold values from -0.125 to 0.125
- shared_w_down: bfloat16 [2816, 2048], P('tp'), may hold values from -0.109375 to 0.109375
Outputs:
- moe_out: bfloat16 [16384, 2048], P('ep', 'tp')
The draws below stay inside these ranges and needn't reach their ends.
Inputs may be any that keep to these rules, and one draw needn't show every extreme that they name: `expert_ids`: each row names 4 different experts below 60. Within the 256 rows of one index of ep no expert is named by more than 32 rows, and in some of these blocks one expert is named by exactly 32 rows.
All inputs are finite; a program needn't handle non-finite values.
Results may differ from the reference program's by a relative error of at most 0.0069.
Values may be sent and summed in bfloat16 or wider, within the bound.
No kernel may reach another device: no remote copies, remote signals or barrier semaphores. Data moves between devices by JAX's collectives and lax.ppermute only.
A program may use at most 128 MiB of HBM per device.

```python
import math
import jax
import jax.numpy as jnp
import numpy as np
from jax import lax

D = 2048
FE = 1408
EXPERTS = 60
TOPK = 4
SF = 2816
TOK_DEV = 256
CAP = 32
SLOTS = 64
TOKENS = 16384
N_EP = 64


def draw_tokens(key, part):
    base = jax.random.fold_in(key, 11)
    first, second = jax.random.split(base, 2)
    noise = jnp.clip(jax.random.normal(first, (TOKENS, D), jnp.float32), -4.0, 4.0)
    rising = 3.0 ** (jnp.arange(D, dtype=jnp.float32) / D)
    column = jnp.exp(jax.random.uniform(second, (D,), jnp.float32, math.log(0.3), 0.0)) * rising
    values = noise * column[None, :]
    return values.astype(jnp.bfloat16)


def draw_router_weight(key, part):
    base = jax.random.fold_in(key, 13)
    values = jnp.clip(jax.random.normal(base, (D, EXPERTS), jnp.float32), -4.0, 4.0) * (0.4 / math.sqrt(D))
    values = jnp.clip(values, -2.0, 2.0)
    return values.astype(jnp.bfloat16)


def block_levels(key, extent, cuts, low, largest):
    loudness, own = 1.0, jax.random.fold_in(key, 6)
    for dim, shards_of in cuts:
        steps = jnp.exp(jax.random.uniform(jax.random.fold_in(own, dim), (shards_of,), jnp.float32, low / len(cuts), largest / len(cuts)))
        loudness = loudness * jnp.repeat(steps, extent[dim] // shards_of).reshape([-1 if axis == dim else 1 for axis in range(len(extent))])
    return loudness


def deal_out(own_key, own, number, rows, amount, top, most, slope):
    sequence = jax.random.permutation(own_key, amount)
    packed, ordinary = load_shares(amount, rows * top, most, slope, True), load_shares(amount, rows * top, most, slope, False)
    places = jnp.arange(amount)

    def named(lengths, rotation):
        used = int((lengths > 0).sum())
        fixed = max(1, used // 4)
        shifted = fixed + (places - fixed + rotation * (used - fixed)) % max(1, amount - fixed)
        return jnp.zeros((amount,), jnp.int32).at[sequence[jnp.where(places < fixed, places, shifted)]].set(jnp.asarray(lengths, jnp.int32))

    lengths = jnp.where(number % 4 == 0, named(packed, number // 4), named(ordinary, number - number // 4 - 1))
    mixed = jax.random.permutation(jax.random.fold_in(own, 3), amount)
    giver, receiver = mixed[0:amount // 2 * 2:2], mixed[1:amount // 2 * 2:2]
    slack = jnp.minimum(lengths[giver] - 1, most - lengths[receiver]) // 2
    slack = jnp.where((giver == sequence[0]) | (receiver == sequence[0]) | (lengths[receiver] == 0), 0, jnp.maximum(slack, 0))
    shifted = jax.random.randint(jax.random.fold_in(own, 4), (amount // 2,), 0, 1 << 20) % (slack + 1)
    lengths = lengths.at[giver].add(-shifted).at[receiver].add(shifted)
    members = jnp.searchsorted(jnp.cumsum(lengths), jnp.arange(rows * top), side="right").astype(jnp.int32)
    table = members.reshape(top, rows).T
    table = table[jax.random.permutation(jax.random.fold_in(own, 1), rows)]
    rotation = jax.random.randint(jax.random.fold_in(own, 2), (rows, 1), 0, top)
    return jnp.take_along_axis(table, (jnp.arange(top)[None, :] + rotation) % top, axis=1)


def load_shares(amount, total, most, lean, full):
    weights = [(1 << 20) // math.isqrt(rank ** lean) + 1 for rank in range(1, amount + 1)]
    largest = most if full else min(most, max(-(-total // amount), total * weights[0] // sum(weights)))
    least = 1 if total - largest >= amount - 1 else 0
    given, rest = [largest] + [least] * (amount - 1), total - largest - least * (amount - 1)
    while rest > 0:
        free = [i for i in range(1, amount) if given[i] < largest] or [i for i in range(1, amount) if given[i] < most]
        mass, budget = sum([weights[i] for i in free]), rest
        for i in free:
            extra = min(most - given[i], max(1, budget * weights[i] // mass), rest)
            given[i] = given[i] + extra
            rest = rest - extra
    return np.array(given)


def centred(key, shape, scale, reach, cuts=(), kind=jnp.bfloat16):
    values = jax.random.normal(key, shape, jnp.float32) * scale
    if len(cuts) > 0:
        values = block_levels(key, shape, cuts, -0.22, 0.18) * values
    return jnp.clip(values, min=-reach, max=reach).astype(kind)


def setup_inputs(seed: int = 0) -> dict:
    key_list = jax.random.split(jax.random.key(seed), 12)
    tokens = draw_tokens(jax.random.fold_in(key_list[11], 71), 0)
    norm_gain = jnp.clip(1.0 + 0.18 * jax.random.normal(key_list[1], (D,), jnp.float32), 0.1, 1.9)
    router_weight = draw_router_weight(jax.random.fold_in(key_list[11], 71), 0)
    shared_gate_w = centred(key_list[3], (D,), D ** -0.5, 0.125)
    expert_ids_keys = jax.random.split(jax.random.fold_in(key_list[4], 1), TOKENS // TOK_DEV)
    expert_ids_turns = jax.random.permutation(jax.random.fold_in(key_list[4], 3), TOKENS // TOK_DEV)
    expert_ids = jax.vmap(lambda own, number: deal_out(jax.random.fold_in(key_list[4], 2), own, number, TOK_DEV, EXPERTS, TOPK, CAP, 2))(expert_ids_keys, expert_ids_turns).reshape((TOKENS, TOPK))
    w_gate = centred(key_list[5], (SLOTS, D, FE), D ** -0.5, 0.125, ((0, 64), (2, 4)))
    w_up = centred(key_list[6], (SLOTS, D, FE), D ** -0.5, 0.125, ((0, 64), (2, 4)))
    w_down = centred(key_list[7], (SLOTS, FE, D), 0.25, 1.5, ((0, 64), (1, 4)))
    shared_w_gate = centred(key_list[8], (D, SF), D ** -0.5, 0.125, ((1, 4),))
    shared_w_up = centred(key_list[9], (D, SF), D ** -0.5, 0.125, ((1, 4),))
    shared_w_down = centred(key_list[10], (SF, D), SF ** -0.5, 0.109375, ((0, 4),))
    return {"tokens": tokens, "norm_gain": norm_gain, "router_weight": router_weight, "shared_gate_w": shared_gate_w, "expert_ids": expert_ids, "w_gate": w_gate, "w_up": w_up, "w_down": w_down, "shared_w_gate": shared_w_gate, "shared_w_up": shared_w_up, "shared_w_down": shared_w_down}


def reference(tokens, norm_gain, router_weight, shared_gate_w, expert_ids, w_gate, w_up, w_down, shared_w_gate, shared_w_up, shared_w_down):
    values = tokens.astype(jnp.float32)
    inv_rms = lax.rsqrt(lax.optimization_barrier(jnp.mean(values * values, axis=-1, keepdims=True)) + 1e-06)
    normed = (values * inv_rms * norm_gain[None, :]).astype(jnp.bfloat16)
    logits = jnp.dot(normed, router_weight, preferred_element_type=jnp.float32)
    probs = jax.nn.softmax(logits, axis=-1)
    route_weight = jnp.take_along_axis(probs, expert_ids, axis=1)
    shared_gate_act = jnp.dot(normed, shared_w_gate, preferred_element_type=jnp.float32)
    shared_up_act = jnp.dot(normed, shared_w_up, preferred_element_type=jnp.float32)
    shared_hidden = (jax.nn.silu(shared_gate_act) * shared_up_act).astype(jnp.bfloat16)
    shared = jnp.dot(shared_hidden, shared_w_down, preferred_element_type=jnp.float32)
    share_gate = jax.nn.sigmoid(jnp.dot(normed, shared_gate_w, preferred_element_type=jnp.float32))
    assigns = TOKENS * TOPK
    blocked = expert_ids.reshape(N_EP, TOK_DEV * TOPK)
    one_hot = (blocked[:, :, None] == jnp.arange(EXPERTS, dtype=jnp.int32)[None, None, :]).astype(jnp.int32)
    before = jnp.cumsum(one_hot, axis=1) - one_hot
    order_rank = lax.optimization_barrier(jnp.sum(before * one_hot, axis=-1))
    position = jnp.arange(N_EP, dtype=jnp.int32)[:, None] * CAP + order_rank
    assign_ids = jnp.arange(assigns, dtype=jnp.int32)
    table = jnp.full((EXPERTS, N_EP * CAP), assigns, jnp.int32)
    table = table.at[blocked.reshape(-1), position.reshape(-1)].set(assign_ids)
    normed_pad = jnp.concatenate([normed, jnp.zeros((1, D), jnp.bfloat16)], axis=0)
    weight_pad = jnp.concatenate([route_weight.reshape(-1), jnp.zeros((1,), jnp.float32)], axis=0)

    def expert_step(total, expert):
        entries = table[expert]
        token_ids = (entries // TOPK).astype(jnp.int32)
        rows = normed_pad[token_ids]
        gate_act = jnp.dot(rows, w_gate[expert], preferred_element_type=jnp.float32)
        up_act = jnp.dot(rows, w_up[expert], preferred_element_type=jnp.float32)
        hidden = (jax.nn.silu(gate_act) * up_act).astype(jnp.bfloat16)
        result = jnp.dot(hidden, w_down[expert], preferred_element_type=jnp.float32).astype(jnp.bfloat16)
        total = total.at[token_ids].add(weight_pad[entries][:, None] * result.astype(jnp.float32))
        return (total, None)
    routed, _ = lax.scan(expert_step, jnp.zeros((TOKENS + 1, D), jnp.float32), jnp.arange(EXPERTS, dtype=jnp.int32))
    return (share_gate[:, None] * shared + routed[:TOKENS]).astype(jnp.bfloat16)
```

```python
import jax
import jax.numpy as jnp
from jax import lax
from jax.experimental import pallas as pl
from jax.experimental.pallas import tpu as pltpu
from jax.sharding import PartitionSpec as P


BF16 = jnp.bfloat16
F32 = jnp.float32
BOTH = ("ep", "tp")
CHUNKS = 2


def pair_perms(mesh):
    ep, tp = mesh.shape["ep"], mesh.shape["tp"]
    near, across = [], []
    for e in range(ep):
        for t in range(tp):
            flip, mirror = t ^ 1, tp - 1 - t
            a, b = (flip, mirror) if e % 2 == 0 else (mirror, flip)
            near.append((e * tp + t, e * tp + a))
            across.append((e * tp + t, e * tp + b))
    return near, across


def dot(a, b, dims=((1,), (0,))):
    return lax.dot_general(a, b, (dims, ((), ())), preferred_element_type=F32)


HBM = pl.BlockSpec(memory_space=pltpu.HBM)
VMEM = pl.BlockSpec(memory_space=pltpu.VMEM)
SMEM = pl.BlockSpec(memory_space=pltpu.SMEM)
BIG = pltpu.CompilerParams(vmem_limit_bytes=60 * 1024 * 1024)
SMALL = pltpu.CompilerParams(vmem_limit_bytes=24 * 1024 * 1024)


def load(pairs, sems):
    copies = [pltpu.make_async_copy(a, b, sems.at[i]) for i, (a, b) in enumerate(pairs)]
    for c in copies:
        c.start()
    return copies


def halves(refs, target):
    units = refs[0].shape[0]
    return [(r, target.at[pl.ds(i * units, units)]) for i, r in enumerate(refs)]


def ffn_kernel(gain, x_in, gate_a, gate_b, up_a, up_b, down_a, down_b, out, xv, x, gate_w, up_w, down_w, y, sems):
    pairs = [(x_in, xv), *halves((gate_a, gate_b), gate_w), *halves((up_a, up_b), up_w)]
    copies = load(pairs + halves((down_a, down_b), down_w), sems)
    rows, full = x.shape
    half = full // 2
    copies[0].wait()
    small = 32
    first = lax.broadcasted_iota(jnp.int32, (small // 8, 8, half), 1) < 4

    def norm_step(i, carry):
        at = pl.ds(pl.multiple_of(i * 2 * small, 2 * small), 2 * small)
        v = xv[at, :].astype(F32)
        shifted = pltpu.roll(v, 4, 0).reshape(small // 8, 2, 8, half)[:, 1]
        v = v.reshape(small // 8, 2, 8, half)
        lower = jnp.where(first, v[:, 0], shifted).reshape(small, half)
        upper = jnp.where(first, shifted, v[:, 1]).reshape(small, half)
        squares = jnp.sum(lower * lower, axis=-1, keepdims=True)
        squares = squares + jnp.sum(upper * upper, axis=-1, keepdims=True)
        inv_rms = lax.rsqrt(squares / full + 1e-06)
        to = pl.ds(pl.multiple_of(i * small, small), small)
        x[to, :half] = (lower * inv_rms * gain[:, :half]).astype(BF16)
        x[to, half:] = (upper * inv_rms * gain[:, half:]).astype(BF16)
        return carry

    lax.fori_loop(0, rows // small, norm_step, 0)
    for c in copies[1:3]:
        c.wait()
    gate = dot(x[...], gate_w[...], ((1,), (1,)))
    for c in copies[3:5]:
        c.wait()
    up = dot(x[...], up_w[...], ((1,), (1,)))
    hidden = (gate / (1.0 + jnp.exp(-gate)) * up).astype(BF16)
    for c in copies[5:]:
        c.wait()
    y[...] = dot(hidden, down_w[...])

    def out_step(i, carry):
        at = pl.ds(pl.multiple_of(i * small, small), small)
        lower, upper = y[at, :half], y[at, half:]
        lower_up = pltpu.roll(lower, small - 4, 0).reshape(small // 8, 8, half)
        upper_down = pltpu.roll(upper, 4, 0).reshape(small // 8, 8, half)
        lower, upper = lower.reshape(small // 8, 8, half), upper.reshape(small // 8, 8, half)
        even, odd = jnp.where(first, lower, upper_down), jnp.where(first, lower_up, upper)
        both = jnp.concatenate([even[:, None], odd[:, None]], axis=1).reshape(2 * small, half)
        to = pl.ds(pl.multiple_of(i * 2 * small, 2 * small), 2 * small)
        out[to, :] = both.astype(out.dtype)
        return carry

    lax.fori_loop(0, rows // small, out_step, 0)


def half_ffn(gain, x, weights, dtype):
    (rows, full), units = (x.shape[0] // 2, x.shape[1] * 2), 2 * weights[0].shape[0]
    return pl.pallas_call(
        ffn_kernel,
        out_shape=jax.ShapeDtypeStruct(x.shape, dtype),
        in_specs=[VMEM] + [HBM] * 7,
        out_specs=VMEM,
        scratch_shapes=[
            pltpu.VMEM(x.shape, BF16),
            pltpu.VMEM((rows, full), BF16),
            *[pltpu.VMEM((units, full), BF16)] * 3,
            pltpu.VMEM((rows, full), F32),
            pltpu.SemaphoreType.DMA((7,)),
        ],
        cost_estimate=pl.CostEstimate(
            flops=6 * rows * full * units,
            transcendentals=rows * units,
            bytes_accessed=2 * (3 * units * full + 2 * rows * full),
        ),
        compiler_params=BIG,
    )(gain, x, *weights)


def dispatch_kernel(starts, pick, part_0, part_1, part_2, part_3, whole, *outs):
    width = part_0.shape[1]
    rows, half = outs[0].shape
    for k, part in enumerate((part_0, part_1, part_2, part_3)):
        whole[:, pl.ds(pl.multiple_of(starts[k], width), width)] = part[...]
    upper_row = lax.broadcasted_iota(jnp.int32, (rows, width), 0) % 8 // 4
    for k, a, b in ((0, part_0, part_3), (1, part_1, part_2)):
        is_a = upper_row == starts[k] // half
        at = pl.ds(pl.multiple_of(starts[k] % half, width), width)
        for c, out in enumerate(outs):
            out[:, at] = jnp.where(is_a, dot(pick[c], a[...]), dot(pick[c], b[...])).astype(BF16)


def dispatched_rows(starts, pick, parts):
    tokens, width = parts[0].shape
    full, rows = width * len(parts), pick.shape[1]
    out = jax.ShapeDtypeStruct((rows, full // 2), BF16)
    return pl.pallas_call(
        dispatch_kernel,
        out_shape=[jax.ShapeDtypeStruct((tokens, full), BF16)] + [out] * CHUNKS,
        in_specs=[SMEM] + [VMEM] * 5,
        out_specs=[VMEM] * (1 + CHUNKS),
        cost_estimate=pl.CostEstimate(
            flops=2 * pick.size * full, transcendentals=0, bytes_accessed=8 * tokens * full
        ),
        compiler_params=SMALL,
    )(starts, pick, *parts)


def gather_kernel(mix_hi, mix_lo, rows, base, out):
    half = rows.shape[1]
    for h in range(2):
        at = slice(h * half, (h + 1) * half)
        out[:, at] = base[:, at] + dot(mix_hi[h], rows[...]) + dot(mix_lo[h], rows[...])


def gathered(mix_hi, mix_lo, rows, base):
    return pl.pallas_call(
        gather_kernel,
        out_shape=jax.ShapeDtypeStruct(base.shape, F32),
        in_specs=[VMEM] * 4,
        out_specs=VMEM,
        cost_estimate=pl.CostEstimate(
            flops=4 * mix_hi.size * rows.shape[1], transcendentals=0, bytes_accessed=8 * base.size
        ),
        compiler_params=SMALL,
    )(mix_hi, mix_lo, rows, base)


def combine_kernel(starts, mix_hi, mix_lo, rows, base, mine, near, across, diag):
    width, half = mine.shape[1], rows.shape[1]
    for k, out in ((3, diag), (2, across), (1, near), (0, mine)):
        h = starts[k] // half
        from_rows = pl.ds(pl.multiple_of(starts[k] % half, width), width)
        value = dot(mix_hi[h], rows[:, from_rows]) + dot(mix_lo[h], rows[:, from_rows])
        at = pl.ds(pl.multiple_of(starts[k], width), width)
        out[...] = (base[:, at] + value).astype(out.dtype)


def combined(starts, mix_hi, mix_lo, rows, base):
    tokens, full = base.shape
    return pl.pallas_call(
        combine_kernel,
        out_shape=[jax.ShapeDtypeStruct((tokens, full // 4), d) for d in (F32, F32, BF16, BF16)],
        in_specs=[SMEM] + [VMEM] * 4,
        out_specs=[VMEM] * 4,
        cost_estimate=pl.CostEstimate(
            flops=4 * mix_hi.size * full // 2, transcendentals=0, bytes_accessed=8 * tokens * full
        ),
        compiler_params=SMALL,
    )(starts, mix_hi, mix_lo, rows, base)


def make(mesh):
    near_pairs, across_pairs = pair_perms(mesh)

    def body(
        tokens,
        norm_gain,
        router_weight,
        shared_gate_w,
        expert_ids,
        w_gate,
        w_up,
        w_down,
        shared_w_gate,
        shared_w_up,
        shared_w_down,
    ):
        rows, width = tokens.shape
        peers = lax.axis_size("tp")
        slots = lax.axis_size("ep")
        full = width * peers
        share = rows // 8 // peers // CHUNKS
        me = lax.axis_index("tp")
        flip, mirror = me ^ 1, peers - 1 - me
        first_core = lax.axis_index("ep") % 2 == 0
        near = jnp.where(first_core, flip, mirror)
        across = jnp.where(first_core, mirror, flip)
        starts = jnp.stack([me, near, across, me ^ 2]).astype(jnp.int32) * width

        def to_near(value):
            return lax.ppermute(value, BOTH, near_pairs)

        def to_across(value):
            return lax.ppermute(value, BOTH, across_pairs)

        def all_parts(value):
            a, b = to_near(value), to_across(value)
            return [value, a, b, to_across(a)]

        parts = all_parts(tokens)
        own_w = (w_gate[0].T, w_up[0].T, w_down[0])
        weights = []
        for w in own_w:
            weights += [w, to_near(w)]

        experts = jnp.arange(slots, dtype=jnp.int32)
        named = jnp.any(expert_ids[:, :, None] == experts[None, None, :], axis=1)
        order = jnp.arange(rows, dtype=jnp.int32)
        earlier = (order[None, :] < order[:, None]).astype(BF16)
        before = dot(earlier, named.astype(BF16))
        key = jnp.where(named, before, -1.0).astype(BF16)
        lane = jnp.arange(slots * 2 * share, dtype=jnp.int32)
        spread = (experts[:, None] == lane[None, :] // (2 * share)).astype(BF16)
        chunk = jnp.arange(CHUNKS, dtype=jnp.int32)
        mine = ((me * CHUNKS + chunk[:, None]) * share + lane[None, :] % share).astype(F32)
        hit = dot(key, spread)[None] == mine[:, None, :]
        pick = (dot(spread, key, ((0,), (1,)))[None] == mine[:, :, None]).astype(BF16)

        whole, *outgoing = dispatched_rows(starts, pick, parts)

        values = whole.astype(F32)
        inv_rms = lax.rsqrt(jnp.mean(values * values, axis=-1, keepdims=True) + 1e-06)
        normed = (values * inv_rms * norm_gain[None, :]).astype(BF16)
        shared_gate_act = dot(normed, shared_w_gate)
        shared_up_act = dot(normed, shared_w_up)
        shared_hidden = (jax.nn.silu(shared_gate_act) * shared_up_act).astype(BF16)
        shared_part = dot(shared_hidden, shared_w_down)
        share_gate = jax.nn.sigmoid(dot(normed, shared_gate_w[:, None]))
        shared_part = lax.optimization_barrier(share_gate * shared_part)

        routers = all_parts(router_weight)
        logits = sum(
            dot(lax.dynamic_slice_in_dim(normed, starts[k], width, 1), r)
            for k, r in enumerate(routers)
        )
        probs = jax.nn.softmax(logits, axis=-1)
        probs = jnp.pad(probs, ((0, 0), (0, slots - probs.shape[1])))
        probs_hi = probs.astype(BF16)
        probs_lo = (probs - probs_hi.astype(F32)).astype(BF16)
        of_half = lane // share % 2 == jnp.arange(2, dtype=jnp.int32)[:, None]
        used = hit[:, None] & of_half[None, :, None, :]
        mix_hi = jnp.where(used, dot(probs_hi, spread)[None, None], 0.0).astype(BF16)
        mix_lo = jnp.where(used, dot(probs_lo, spread)[None, None], 0.0).astype(BF16)
        mixes = [(mix_hi[c], mix_lo[c]) for c in range(CHUNKS)]
        mixes = lax.optimization_barrier(mixes)

        gain = norm_gain[None, :]
        acc = shared_part
        for c in range(CHUNKS):
            there = outgoing[c].reshape(slots, 2 * share, full // 2)
            arrived = lax.all_to_all(there, "ep", 0, 0, tiled=True)
            arrived = arrived.reshape(outgoing[c].shape)
            arrived_far = to_across(arrived)
            sent = half_ffn(gain, arrived_far, weights, BF16)
            got = to_across(sent)
            kept = half_ffn(gain, arrived, weights, F32)
            out = (kept + got.astype(F32)).astype(BF16).reshape(there.shape)
            returned = lax.all_to_all(out, "ep", 0, 0, tiled=True)
            returned = returned.reshape(outgoing[c].shape)
            if c < CHUNKS - 1:
                acc = gathered(*mixes[c], returned, acc)
            else:
                total_me, total_near, for_across, for_diag = combined(starts, *mixes[c], returned, acc)
        came_near = to_across(for_diag)
        came_me = to_across(for_across)
        again = to_near((total_near + came_near.astype(F32)).astype(BF16))
        return (total_me + came_me.astype(F32) + again.astype(F32)).astype(BF16)

    return body


def solution(mesh):
    return jax.shard_map(
        make(mesh),
        mesh=mesh,
        in_specs=(
            P("ep", "tp"),
            P(),
            P("tp", None),
            P(),
            P("ep", None),
            P("ep", None, "tp"),
            P("ep", None, "tp"),
            P("ep", "tp", None),
            P(None, "tp"),
            P(None, "tp"),
            P("tp", None),
        ),
        out_specs=P("ep", "tp"),
        check_vma=False,
    )
```

```python
import jax
import jax.numpy as jnp
from jax import lax
from jax.experimental import pallas as pl
from jax.experimental.pallas import tpu as pltpu
from jax.sharding import PartitionSpec as P


BF16 = jnp.bfloat16
F32 = jnp.float32
BOTH = ("ep", "tp")
CHUNKS = 2


def pair_perms(mesh):
    ep, tp = mesh.shape["ep"], mesh.shape["tp"]
    near, across = [], []
    for e in range(ep):
        for t in range(tp):
            flip, mirror = t ^ 1, tp - 1 - t
            a, b = (flip, mirror) if e % 2 == 0 else (mirror, flip)
            near.append((e * tp + t, e * tp + a))
            across.append((e * tp + t, e * tp + b))
    return near, across


def dot(a, b, dims=((1,), (0,))):
    return lax.dot_general(a, b, (dims, ((), ())), preferred_element_type=F32)


HBM = pl.BlockSpec(memory_space=pltpu.HBM)
VMEM = pl.BlockSpec(memory_space=pltpu.VMEM)
SMEM = pl.BlockSpec(memory_space=pltpu.SMEM)
BIG = pltpu.CompilerParams(vmem_limit_bytes=60 * 1024 * 1024)


def load(pairs, sems):
    copies = [pltpu.make_async_copy(a, b, sems.at[i]) for i, (a, b) in enumerate(pairs)]
    for c in copies:
        c.start()
    return copies


def halves(refs, target):
    units = refs[0].shape[0]
    return [(r, target.at[pl.ds(i * units, units)]) for i, r in enumerate(refs)]


def ffn_kernel(gain, x_in, gate_a, gate_b, up_a, up_b, down_a, down_b, out, xv, x, gate_w, up_w, down_w, y, sems):
    rows, full = x.shape
    half = full // 2
    load([(x_in, xv)], sems)[0].wait()
    pairs = halves((gate_a, gate_b), gate_w) + halves((up_a, up_b), up_w) + halves((down_a, down_b), down_w)
    copies = load(pairs, sems)
    small = 32
    first = lax.broadcasted_iota(jnp.int32, (small // 8, 8, half), 1) < 4

    def norm_step(i, carry):
        at = pl.ds(pl.multiple_of(i * 2 * small, 2 * small), 2 * small)
        v = xv[at, :].astype(F32)
        shifted = pltpu.roll(v, 4, 0).reshape(small // 8, 2, 8, half)[:, 1]
        v = v.reshape(small // 8, 2, 8, half)
        lower = jnp.where(first, v[:, 0], shifted).reshape(small, half)
        upper = jnp.where(first, shifted, v[:, 1]).reshape(small, half)
        squares = jnp.sum(lower * lower, axis=-1, keepdims=True)
        squares = squares + jnp.sum(upper * upper, axis=-1, keepdims=True)
        inv_rms = lax.rsqrt(squares / full + 1e-06)
        to = pl.ds(pl.multiple_of(i * small, small), small)
        x[to, :half] = (lower * inv_rms * gain[:, :half]).astype(BF16)
        x[to, half:] = (upper * inv_rms * gain[:, half:]).astype(BF16)
        return carry

    lax.fori_loop(0, rows // small, norm_step, 0)
    for c in copies[:2]:
        c.wait()
    gate = dot(x[...], gate_w[...], ((1,), (1,)))
    for c in copies[2:4]:
        c.wait()
    up = dot(x[...], up_w[...], ((1,), (1,)))
    hidden = (gate / (1.0 + jnp.exp(-gate)) * up).astype(BF16)
    for c in copies[4:]:
        c.wait()
    y[...] = dot(hidden, down_w[...])

    def out_step(i, carry):
        at = pl.ds(pl.multiple_of(i * small, small), small)
        lower, upper = y[at, :half], y[at, half:]
        lower_up = pltpu.roll(lower, small - 4, 0).reshape(small // 8, 8, half)
        upper_down = pltpu.roll(upper, 4, 0).reshape(small // 8, 8, half)
        lower, upper = lower.reshape(small // 8, 8, half), upper.reshape(small // 8, 8, half)
        even, odd = jnp.where(first, lower, upper_down), jnp.where(first, lower_up, upper)
        both = jnp.concatenate([even[:, None], odd[:, None]], axis=1).reshape(2 * small, half)
        to = pl.ds(pl.multiple_of(i * 2 * small, 2 * small), 2 * small)
        out[to, :] = both.astype(out.dtype)
        return carry

    lax.fori_loop(0, rows // small, out_step, 0)


def half_ffn(gain, x, weights, dtype):
    (rows, full), units = (x.shape[0] // 2, x.shape[1] * 2), 2 * weights[0].shape[0]
    return pl.pallas_call(
        ffn_kernel,
        out_shape=jax.ShapeDtypeStruct(x.shape, dtype),
        in_specs=[VMEM] + [HBM] * 7,
        out_specs=VMEM,
        scratch_shapes=[
            pltpu.VMEM(x.shape, BF16),
            pltpu.VMEM((rows, full), BF16),
            *[pltpu.VMEM((units, full), BF16)] * 3,
            pltpu.VMEM((rows, full), F32),
            pltpu.SemaphoreType.DMA((6,)),
        ],
        cost_estimate=pl.CostEstimate(
            flops=6 * rows * full * units,
            transcendentals=rows * units,
            bytes_accessed=2 * (3 * units * full + 2 * rows * full),
        ),
        compiler_params=BIG,
    )(gain, x, *weights)


def dispatch_kernel(starts, pick, part_0, part_1, part_2, part_3, out, *whole):
    width = part_0.shape[1]
    rows, half = out.shape
    upper_row = lax.broadcasted_iota(jnp.int32, (rows, width), 0) % 8 // 4
    for k, a, b in ((0, part_0, part_3), (1, part_1, part_2)):
        is_a = upper_row == starts[k] // half
        at = pl.ds(pl.multiple_of(starts[k] % half, width), width)
        out[:, at] = jnp.where(is_a, dot(pick[...], a[...]), dot(pick[...], b[...])).astype(BF16)
    for w in whole:
        for k, part in enumerate((part_0, part_1, part_2, part_3)):
            w[:, pl.ds(pl.multiple_of(starts[k], width), width)] = part[...]


def dispatched_rows(starts, pick, parts, with_tokens):
    tokens, width = parts[0].shape
    full, rows = width * len(parts), pick.shape[0]
    shapes = [(rows, full // 2)] + [(tokens, full)] * with_tokens
    return pl.pallas_call(
        dispatch_kernel,
        out_shape=[jax.ShapeDtypeStruct(shape, BF16) for shape in shapes],
        in_specs=[SMEM] + [VMEM] * 5,
        out_specs=[VMEM] * len(shapes),
        cost_estimate=pl.CostEstimate(
            flops=2 * pick.size * full, transcendentals=0, bytes_accessed=4 * tokens * full
        ),
        compiler_params=BIG,
    )(starts, pick, *parts)


def join_kernel(kept, got, out):
    out[...] = (kept[...] + got[...].astype(F32)).astype(BF16)


def joined(kept, got):
    rows, half = kept.shape
    block = pl.BlockSpec((rows // 4, half), lambda i: (i, 0))
    return pl.pallas_call(
        join_kernel,
        out_shape=jax.ShapeDtypeStruct(kept.shape, BF16),
        grid=(4,),
        in_specs=[block] * 2,
        out_specs=block,
        cost_estimate=pl.CostEstimate(flops=kept.size, transcendentals=0, bytes_accessed=8 * kept.size),
        compiler_params=BIG,
    )(kept, got)


def gather_kernel(mix_hi, mix_lo, rows, base, out):
    half = rows.shape[1]
    for h in range(2):
        at = slice(h * half, (h + 1) * half)
        out[:, at] = base[:, at] + dot(mix_hi[h], rows[...]) + dot(mix_lo[h], rows[...])


def gathered(mix_hi, mix_lo, rows, base):
    return pl.pallas_call(
        gather_kernel,
        out_shape=jax.ShapeDtypeStruct(base.shape, F32),
        in_specs=[VMEM] * 4,
        out_specs=VMEM,
        cost_estimate=pl.CostEstimate(
            flops=4 * mix_hi.size * rows.shape[1], transcendentals=0, bytes_accessed=8 * base.size
        ),
        compiler_params=BIG,
    )(mix_hi, mix_lo, rows, base)


def combine_kernel(starts, mix_hi, mix_lo, rows, base, *outs):
    width, half = outs[0].shape[1], rows.shape[1]
    for k, out in enumerate(outs):
        h = starts[k] // half
        from_rows = pl.ds(pl.multiple_of(starts[k] % half, width), width)
        value = dot(mix_hi[h], rows[:, from_rows]) + dot(mix_lo[h], rows[:, from_rows])
        at = pl.ds(pl.multiple_of(starts[k], width), width)
        out[...] = (base[:, at] + value).astype(out.dtype)


def combined(starts, mix_hi, mix_lo, rows, base, dtype):
    tokens, full = base.shape
    count = starts.shape[0]
    return pl.pallas_call(
        combine_kernel,
        out_shape=[jax.ShapeDtypeStruct((tokens, full // 4), dtype)] * count,
        in_specs=[SMEM] + [VMEM] * 4,
        out_specs=[VMEM] * count,
        cost_estimate=pl.CostEstimate(
            flops=mix_hi.size * full, transcendentals=0, bytes_accessed=8 * tokens * full
        ),
        compiler_params=BIG,
    )(starts, mix_hi, mix_lo, rows, base)


def make(mesh):
    near_pairs, across_pairs = pair_perms(mesh)

    def body(
        tokens,
        norm_gain,
        router_weight,
        shared_gate_w,
        expert_ids,
        w_gate,
        w_up,
        w_down,
        shared_w_gate,
        shared_w_up,
        shared_w_down,
    ):
        rows, width = tokens.shape
        peers = lax.axis_size("tp")
        slots = lax.axis_size("ep")
        full = width * peers
        share = rows // 8 // peers // CHUNKS
        me = lax.axis_index("tp")
        flip, mirror = me ^ 1, peers - 1 - me
        first_core = lax.axis_index("ep") % 2 == 0
        near = jnp.where(first_core, flip, mirror)
        across = jnp.where(first_core, mirror, flip)
        starts = jnp.stack([me, near, across, me ^ 2]).astype(jnp.int32) * width

        def to_near(value):
            return lax.ppermute(value, BOTH, near_pairs)

        def to_across(value):
            return lax.ppermute(value, BOTH, across_pairs)

        def all_parts(value):
            a, b = to_near(value), to_across(value)
            return [value, a, b, to_across(a)]

        parts = all_parts(tokens)
        own_w = (w_gate[0].T, w_up[0].T, w_down[0])
        weights = []
        for w in own_w:
            weights += [w, to_near(w)]

        experts = jnp.arange(slots, dtype=jnp.int32)
        named = jnp.any(expert_ids[:, :, None] == experts[None, None, :], axis=1)
        order = jnp.arange(rows, dtype=jnp.int32)
        earlier = (order[None, :] < order[:, None]).astype(BF16)
        before = dot(earlier, named.astype(BF16))
        key = jnp.where(named, before, -1.0).astype(BF16)
        lane = jnp.arange(slots * 2 * share, dtype=jnp.int32)
        spread = (experts[:, None] == lane[None, :] // (2 * share)).astype(BF16)
        chunk = jnp.arange(CHUNKS, dtype=jnp.int32)
        mine = ((me * CHUNKS + chunk[:, None]) * share + lane[None, :] % share).astype(F32)
        hit = dot(key, spread)[None] == mine[:, None, :]
        pick = (dot(spread, key, ((0,), (1,)))[None] == mine[:, :, None]).astype(BF16)

        (outgoing_0,) = dispatched_rows(starts, pick[0], parts, False)
        outgoing_1, whole = dispatched_rows(starts, pick[1], parts, True)
        outgoing = (outgoing_0, outgoing_1)

        values = whole.astype(F32)
        inv_rms = lax.rsqrt(jnp.mean(values * values, axis=-1, keepdims=True) + 1e-06)
        normed = (values * inv_rms * norm_gain[None, :]).astype(BF16)
        shared_gate_act = dot(normed, shared_w_gate)
        shared_up_act = dot(normed, shared_w_up)
        shared_hidden = (jax.nn.silu(shared_gate_act) * shared_up_act).astype(BF16)
        shared_part = dot(shared_hidden, shared_w_down)
        share_gate = jax.nn.sigmoid(dot(normed, shared_gate_w[:, None]))
        shared_part = lax.optimization_barrier(share_gate * shared_part)

        routers = all_parts(router_weight)
        logits = sum(
            dot(lax.dynamic_slice_in_dim(normed, starts[k], width, 1), r)
            for k, r in enumerate(routers)
        )
        probs = jax.nn.softmax(logits, axis=-1)
        probs = jnp.pad(probs, ((0, 0), (0, slots - probs.shape[1])))
        probs_hi = probs.astype(BF16)
        probs_lo = (probs - probs_hi.astype(F32)).astype(BF16)
        of_half = lane // share % 2 == jnp.arange(2, dtype=jnp.int32)[:, None]
        used = hit[:, None] & of_half[None, :, None, :]
        mix_hi = jnp.where(used, dot(probs_hi, spread)[None, None], 0.0).astype(BF16)
        mix_lo = jnp.where(used, dot(probs_lo, spread)[None, None], 0.0).astype(BF16)
        mixes = [(mix_hi[c], mix_lo[c]) for c in range(CHUNKS)]
        mixes = lax.optimization_barrier(mixes)

        gain = norm_gain[None, :]
        acc = shared_part
        for c in range(CHUNKS):
            there = outgoing[c].reshape(slots, 2 * share, full // 2)
            arrived = lax.all_to_all(there, "ep", 0, 0, tiled=True)
            arrived = arrived.reshape(outgoing[c].shape)
            arrived_far = to_across(arrived)
            sent = half_ffn(gain, arrived_far, weights, BF16)
            got = to_across(sent)
            kept = half_ffn(gain, arrived, weights, F32)
            out = joined(kept, got).reshape(there.shape)
            returned = lax.all_to_all(out, "ep", 0, 0, tiled=True)
            returned = returned.reshape(outgoing[c].shape)
            if c < CHUNKS - 1:
                acc = gathered(*mixes[c], returned, acc)
            else:
                for_diag, for_across = combined(starts[:1:-1], *mixes[c], returned, acc, BF16)
                total_near, total_me = combined(starts[1::-1], *mixes[c], returned, acc, F32)
        came_near = to_across(for_diag)
        came_me = to_across(for_across)
        again = to_near((total_near + came_near.astype(F32)).astype(BF16))
        return (total_me + came_me.astype(F32) + again.astype(F32)).astype(BF16)

    return body


def solution(mesh):
    return jax.shard_map(
        make(mesh),
        mesh=mesh,
        in_specs=(
            P("ep", "tp"),
            P(),
            P("tp", None),
            P(),
            P("ep", None),
            P("ep", None, "tp"),
            P("ep", None, "tp"),
            P("ep", "tp", None),
            P(None, "tp"),
            P(None, "tp"),
            P("tp", None),
        ),
        out_specs=P("ep", "tp"),
        check_vma=False,
    )
```

```python
import functools

import jax
import jax.numpy as jnp
from jax import lax
from jax.experimental import pallas as pl
from jax.experimental.pallas import tpu as pltpu
from jax.sharding import PartitionSpec as P


BF16 = jnp.bfloat16
F32 = jnp.float32
BOTH = ("ep", "tp")
CHUNKS = 2


def pair_perms(mesh):
    ep, tp = mesh.shape["ep"], mesh.shape["tp"]
    near, across = [], []
    for e in range(ep):
        for t in range(tp):
            flip, mirror = t ^ 1, tp - 1 - t
            a, b = (flip, mirror) if e % 2 == 0 else (mirror, flip)
            near.append((e * tp + t, e * tp + a))
            across.append((e * tp + t, e * tp + b))
    return near, across


def dot(a, b, dims=((1,), (0,))):
    return lax.dot_general(a, b, (dims, ((), ())), preferred_element_type=F32)


HBM = pl.BlockSpec(memory_space=pltpu.HBM)
VMEM = pl.BlockSpec(memory_space=pltpu.VMEM)
SMEM = pl.BlockSpec(memory_space=pltpu.SMEM)
BIG = pltpu.CompilerParams(vmem_limit_bytes=60 * 1024 * 1024)


def load(pairs, sems):
    copies = [pltpu.make_async_copy(a, b, sems.at[i]) for i, (a, b) in enumerate(pairs)]
    for c in copies:
        c.start()
    return copies


def halves(refs, target):
    units = refs[0].shape[0]
    return [(r, target.at[pl.ds(i * units, units)]) for i, r in enumerate(refs)]


def ffn_kernel(gain_in, x_in, gate_a, gate_b, up_a, up_b, down_a, down_b, out, gain, xv, x, gate_w, up_w, down_w, y, sems):
    rows, full = x.shape
    half = full // 2
    pairs = [(x_in, xv), (gain_in, gain), *halves((gate_a, gate_b), gate_w), *halves((up_a, up_b), up_w)]
    copies = load(pairs + halves((down_a, down_b), down_w), sems)
    for c in copies[:2]:
        c.wait()
    small = 32
    first = lax.broadcasted_iota(jnp.int32, (small // 8, 8, half), 1) < 4

    def norm_step(i, carry):
        at = pl.ds(pl.multiple_of(i * 2 * small, 2 * small), 2 * small)
        v = xv[at, :].astype(F32)
        shifted = pltpu.roll(v, 4, 0).reshape(small // 8, 2, 8, half)[:, 1]
        v = v.reshape(small // 8, 2, 8, half)
        lower = jnp.where(first, v[:, 0], shifted).reshape(small, half)
        upper = jnp.where(first, shifted, v[:, 1]).reshape(small, half)
        squares = jnp.sum(lower * lower, axis=-1, keepdims=True)
        squares = squares + jnp.sum(upper * upper, axis=-1, keepdims=True)
        inv_rms = lax.rsqrt(squares / full + 1e-06)
        to = pl.ds(pl.multiple_of(i * small, small), small)
        x[to, :half] = (lower * inv_rms * gain[:, :half]).astype(BF16)
        x[to, half:] = (upper * inv_rms * gain[:, half:]).astype(BF16)
        return carry

    lax.fori_loop(0, rows // small, norm_step, 0)
    for c in copies[2:4]:
        c.wait()
    gate = dot(x[...], gate_w[...], ((1,), (1,)))
    for c in copies[4:6]:
        c.wait()
    up = dot(x[...], up_w[...], ((1,), (1,)))
    hidden = (gate / (1.0 + jnp.exp(-gate)) * up).astype(BF16)
    for c in copies[6:]:
        c.wait()
    y[...] = dot(hidden, down_w[...])

    def out_step(i, carry):
        at = pl.ds(pl.multiple_of(i * small, small), small)
        lower, upper = y[at, :half], y[at, half:]
        lower_up = pltpu.roll(lower, small - 4, 0).reshape(small // 8, 8, half)
        upper_down = pltpu.roll(upper, 4, 0).reshape(small // 8, 8, half)
        lower, upper = lower.reshape(small // 8, 8, half), upper.reshape(small // 8, 8, half)
        even, odd = jnp.where(first, lower, upper_down), jnp.where(first, lower_up, upper)
        both = jnp.concatenate([even[:, None], odd[:, None]], axis=1).reshape(2 * small, half)
        to = pl.ds(pl.multiple_of(i * 2 * small, 2 * small), 2 * small)
        out[to, :] = both.astype(out.dtype)
        return carry

    lax.fori_loop(0, rows // small, out_step, 0)


def half_ffn(gain, x, weights):
    (rows, full), units = (x.shape[0] // 2, x.shape[1] * 2), 2 * weights[0].shape[0]
    return pl.pallas_call(
        ffn_kernel,
        out_shape=jax.ShapeDtypeStruct(x.shape, BF16),
        in_specs=[HBM] * 8,
        out_specs=VMEM,
        scratch_shapes=[
            pltpu.VMEM(gain.shape, F32),
            pltpu.VMEM(x.shape, BF16),
            pltpu.VMEM((rows, full), BF16),
            *[pltpu.VMEM((units, full), BF16)] * 3,
            pltpu.VMEM((rows, full), F32),
            pltpu.SemaphoreType.DMA((8,)),
        ],
        cost_estimate=pl.CostEstimate(
            flops=6 * rows * full * units,
            transcendentals=rows * units,
            bytes_accessed=2 * (3 * units * full + 2 * rows * full),
        ),
        compiler_params=BIG,
    )(gain, x, *weights)


def dispatch_kernel(starts, pick, part_0, part_1, part_2, part_3, out, *whole):
    width = part_0.shape[1]
    rows, half = out.shape
    upper_row = lax.broadcasted_iota(jnp.int32, (rows, width), 0) % 8 // 4
    for k, a, b in ((0, part_0, part_3), (1, part_1, part_2)):
        is_a = upper_row == starts[k] // half
        at = pl.ds(pl.multiple_of(starts[k] % half, width), width)
        out[:, at] = jnp.where(is_a, dot(pick[...], a[...]), dot(pick[...], b[...])).astype(BF16)
    for w in whole:
        for k, part in enumerate((part_0, part_1, part_2, part_3)):
            w[:, pl.ds(pl.multiple_of(starts[k], width), width)] = part[...]


def dispatched_rows(starts, pick, parts, with_tokens):
    tokens, width = parts[0].shape
    full, rows = width * len(parts), pick.shape[0]
    shapes = [(rows, full // 2)] + [(tokens, full)] * with_tokens
    return pl.pallas_call(
        dispatch_kernel,
        out_shape=[jax.ShapeDtypeStruct(shape, BF16) for shape in shapes],
        in_specs=[SMEM] + [VMEM] * 5,
        out_specs=[VMEM] * len(shapes),
        cost_estimate=pl.CostEstimate(
            flops=2 * pick.size * full, transcendentals=0, bytes_accessed=4 * tokens * full
        ),
        compiler_params=BIG,
    )(starts, pick, *parts)


def gather_kernel(mix_hi, mix_lo, rows, base, out):
    half = rows.shape[1]
    for h in range(2):
        at = slice(h * half, (h + 1) * half)
        out[:, at] = base[:, at] + dot(mix_hi[h], rows[...]) + dot(mix_lo[h], rows[...])


def gathered(mix_hi, mix_lo, rows, base):
    return pl.pallas_call(
        gather_kernel,
        out_shape=jax.ShapeDtypeStruct(base.shape, F32),
        in_specs=[VMEM] * 4,
        out_specs=VMEM,
        cost_estimate=pl.CostEstimate(
            flops=4 * mix_hi.size * rows.shape[1], transcendentals=0, bytes_accessed=8 * base.size
        ),
        compiler_params=BIG,
    )(mix_hi, mix_lo, rows, base)


def combine_kernel(starts, mix_hi, mix_lo, rows, base, *outs, parts):
    width, half = outs[0].shape[1], rows.shape[1]
    for k, out in zip(parts, outs):
        h = starts[k] // half
        from_rows = pl.ds(pl.multiple_of(starts[k] % half, width), width)
        value = dot(mix_hi[h], rows[:, from_rows]) + dot(mix_lo[h], rows[:, from_rows])
        at = pl.ds(pl.multiple_of(starts[k], width), width)
        out[...] = (base[:, at] + value).astype(out.dtype)


def combined(starts, parts, mix_hi, mix_lo, rows, base, dtype):
    tokens, full = base.shape
    count = len(parts)
    return pl.pallas_call(
        functools.partial(combine_kernel, parts=parts),
        out_shape=[jax.ShapeDtypeStruct((tokens, full // 4), dtype)] * count,
        in_specs=[SMEM] + [VMEM] * 4,
        out_specs=[VMEM] * count,
        cost_estimate=pl.CostEstimate(
            flops=mix_hi.size * full, transcendentals=0, bytes_accessed=8 * tokens * full
        ),
        compiler_params=BIG,
    )(starts, mix_hi, mix_lo, rows, base)


def make(mesh):
    near_pairs, across_pairs = pair_perms(mesh)

    def body(
        tokens,
        norm_gain,
        router_weight,
        shared_gate_w,
        expert_ids,
        w_gate,
        w_up,
        w_down,
        shared_w_gate,
        shared_w_up,
        shared_w_down,
    ):
        rows, width = tokens.shape
        peers = lax.axis_size("tp")
        slots = lax.axis_size("ep")
        full = width * peers
        share = rows // 8 // peers // CHUNKS
        me = lax.axis_index("tp")
        flip, mirror = me ^ 1, peers - 1 - me
        first_core = lax.axis_index("ep") % 2 == 0
        near = jnp.where(first_core, flip, mirror)
        across = jnp.where(first_core, mirror, flip)
        starts = jnp.stack([me, near, across, me ^ 2]).astype(jnp.int32) * width

        def to_near(value):
            return lax.ppermute(value, BOTH, near_pairs)

        def to_across(value):
            return lax.ppermute(value, BOTH, across_pairs)

        def all_parts(value):
            a, b = to_near(value), to_across(value)
            return [value, a, b, to_across(a)]

        parts = all_parts(tokens)
        own_w = (w_gate[0].T, w_up[0].T, w_down[0])
        weights = []
        for w in own_w:
            weights += [w, to_near(w)]

        experts = jnp.arange(slots, dtype=jnp.int32)
        named = jnp.any(expert_ids[:, :, None] == experts[None, None, :], axis=1)
        order = jnp.arange(rows, dtype=jnp.int32)
        earlier = (order[None, :] < order[:, None]).astype(BF16)
        before = dot(earlier, named.astype(BF16))
        key = jnp.where(named, before, -1.0).astype(BF16)
        lane = jnp.arange(slots * 2 * share, dtype=jnp.int32)
        spread = (experts[:, None] == lane[None, :] // (2 * share)).astype(BF16)
        chunk = jnp.arange(CHUNKS, dtype=jnp.int32)
        mine = ((me * CHUNKS + chunk[:, None]) * share + lane[None, :] % share).astype(F32)
        hit = dot(key, spread)[None] == mine[:, None, :]
        pick = (dot(spread, key, ((0,), (1,)))[None] == mine[:, :, None]).astype(BF16)

        (outgoing_0,) = dispatched_rows(starts, pick[0], parts, False)
        outgoing_1, whole = dispatched_rows(starts, pick[1], parts, True)
        outgoing = (outgoing_0, outgoing_1)

        values = whole.astype(F32)
        inv_rms = lax.rsqrt(jnp.mean(values * values, axis=-1, keepdims=True) + 1e-06)
        normed = (values * inv_rms * norm_gain[None, :]).astype(BF16)
        shared_gate_act = dot(normed, shared_w_gate)
        shared_up_act = dot(normed, shared_w_up)
        shared_hidden = (jax.nn.silu(shared_gate_act) * shared_up_act).astype(BF16)
        shared_part = dot(shared_hidden, shared_w_down)
        share_gate = jax.nn.sigmoid(dot(normed, shared_gate_w[:, None]))
        shared_part = lax.optimization_barrier(share_gate * shared_part)

        routers = all_parts(router_weight)
        logits = sum(
            dot(lax.dynamic_slice_in_dim(normed, starts[k], width, 1), r)
            for k, r in enumerate(routers)
        )
        probs = jax.nn.softmax(logits, axis=-1)
        probs = jnp.pad(probs, ((0, 0), (0, slots - probs.shape[1])))
        probs_hi = probs.astype(BF16)
        probs_lo = (probs - probs_hi.astype(F32)).astype(BF16)
        of_half = lane // share % 2 == jnp.arange(2, dtype=jnp.int32)[:, None]
        used = hit[:, None] & of_half[None, :, None, :]
        mix_hi = jnp.where(used, dot(probs_hi, spread)[None, None], 0.0).astype(BF16)
        mix_lo = jnp.where(used, dot(probs_lo, spread)[None, None], 0.0).astype(BF16)
        mixes = [(mix_hi[c], mix_lo[c]) for c in range(CHUNKS)]
        mixes = lax.optimization_barrier(mixes)

        gain = norm_gain[None, :]
        acc = shared_part
        for c in range(CHUNKS):
            there = outgoing[c].reshape(slots, 2 * share, full // 2)
            arrived = lax.all_to_all(there, "ep", 0, 0, tiled=True)
            arrived = arrived.reshape(outgoing[c].shape)
            arrived_far = to_across(arrived)
            sent = half_ffn(gain, arrived_far, weights)
            got = to_across(sent)
            kept = half_ffn(gain, arrived, weights)
            out = (kept.astype(F32) + got.astype(F32)).astype(BF16).reshape(there.shape)
            returned = lax.all_to_all(out, "ep", 0, 0, tiled=True)
            returned = returned.reshape(outgoing[c].shape)
            if c < CHUNKS - 1:
                acc = gathered(*mixes[c], returned, acc)
            else:
                for_diag, for_across = combined(starts, (3, 2), *mixes[c], returned, acc, BF16)
                total_near, total_me = combined(starts, (1, 0), *mixes[c], returned, acc, F32)
        came_near = to_across(for_diag)
        came_me = to_across(for_across)
        again = to_near((total_near + came_near.astype(F32)).astype(BF16))
        return (total_me + came_me.astype(F32) + again.astype(F32)).astype(BF16)

    return body


def solution(mesh):
    return jax.shard_map(
        make(mesh),
        mesh=mesh,
        in_specs=(
            P("ep", "tp"),
            P(),
            P("tp", None),
            P(),
            P("ep", None),
            P("ep", None, "tp"),
            P("ep", None, "tp"),
            P("ep", "tp", None),
            P(None, "tp"),
            P(None, "tp"),
            P("tp", None),
        ),
        out_specs=P("ep", "tp"),
        check_vma=False,
    )
```

```python
import functools

import jax
import jax.numpy as jnp
from jax import lax
from jax.experimental import pallas as pl
from jax.experimental.pallas import tpu as pltpu
from jax.sharding import PartitionSpec as P


BF16 = jnp.bfloat16
F32 = jnp.float32
BOTH = ("ep", "tp")
CHUNKS = 2


def pair_perms(mesh):
    ep, tp = mesh.shape["ep"], mesh.shape["tp"]
    near, across, diag = [], [], []
    for e in range(ep):
        for t in range(tp):
            flip, mirror = t ^ 1, tp - 1 - t
            a, b = (flip, mirror) if e % 2 == 0 else (mirror, flip)
            near.append((e * tp + t, e * tp + a))
            across.append((e * tp + t, e * tp + b))
            diag.append((e * tp + t, e * tp + (t ^ 2)))
    return near, across, diag


def dot(a, b, dims=((1,), (0,))):
    return lax.dot_general(a, b, (dims, ((), ())), preferred_element_type=F32)


HBM = pl.BlockSpec(memory_space=pltpu.HBM)
VMEM = pl.BlockSpec(memory_space=pltpu.VMEM)
SMEM = pl.BlockSpec(memory_space=pltpu.SMEM)
BIG = pltpu.CompilerParams(vmem_limit_bytes=60 * 1024 * 1024)


def load(pairs, sems):
    copies = [pltpu.make_async_copy(a, b, sems.at[i]) for i, (a, b) in enumerate(pairs)]
    for c in copies:
        c.start()
    return copies


def halves(refs, target):
    units = refs[0].shape[0]
    return [(r, target.at[pl.ds(i * units, units)]) for i, r in enumerate(refs)]


def ffn_kernel(gain_in, x_in, gate_a, gate_b, up_a, up_b, down_a, down_b, out, gain, xv, x, gate_w, up_w, down_w, y, sems):
    rows, full = x.shape
    half = full // 2
    pairs = [(x_in, xv), (gain_in, gain), *halves((gate_a, gate_b), gate_w), *halves((up_a, up_b), up_w)]
    copies = load(pairs + halves((down_a, down_b), down_w), sems)
    for c in copies[:2]:
        c.wait()
    small = 32
    first = lax.broadcasted_iota(jnp.int32, (small // 8, 8, half), 1) < 4

    def norm_step(i, carry):
        at = pl.ds(pl.multiple_of(i * 2 * small, 2 * small), 2 * small)
        v = xv[at, :].astype(F32)
        shifted = pltpu.roll(v, 4, 0).reshape(small // 8, 2, 8, half)[:, 1]
        v = v.reshape(small // 8, 2, 8, half)
        lower = jnp.where(first, v[:, 0], shifted).reshape(small, half)
        upper = jnp.where(first, shifted, v[:, 1]).reshape(small, half)
        squares = jnp.sum(lower * lower, axis=-1, keepdims=True)
        squares = squares + jnp.sum(upper * upper, axis=-1, keepdims=True)
        inv_rms = lax.rsqrt(squares / full + 1e-06)
        to = pl.ds(pl.multiple_of(i * small, small), small)
        x[to, :half] = (lower * inv_rms * gain[:, :half]).astype(BF16)
        x[to, half:] = (upper * inv_rms * gain[:, half:]).astype(BF16)
        return carry

    lax.fori_loop(0, rows // small, norm_step, 0)
    for c in copies[2:4]:
        c.wait()
    gate = dot(x[...], gate_w[...], ((1,), (1,)))
    for c in copies[4:6]:
        c.wait()
    up = dot(x[...], up_w[...], ((1,), (1,)))
    hidden = (gate / (1.0 + jnp.exp(-gate)) * up).astype(BF16)
    for c in copies[6:]:
        c.wait()
    y[...] = dot(hidden, down_w[...])

    def out_step(i, carry):
        at = pl.ds(pl.multiple_of(i * small, small), small)
        lower, upper = y[at, :half], y[at, half:]
        lower_up = pltpu.roll(lower, small - 4, 0).reshape(small // 8, 8, half)
        upper_down = pltpu.roll(upper, 4, 0).reshape(small // 8, 8, half)
        lower, upper = lower.reshape(small // 8, 8, half), upper.reshape(small // 8, 8, half)
        even, odd = jnp.where(first, lower, upper_down), jnp.where(first, lower_up, upper)
        both = jnp.concatenate([even[:, None], odd[:, None]], axis=1).reshape(2 * small, half)
        to = pl.ds(pl.multiple_of(i * 2 * small, 2 * small), 2 * small)
        out[to, :] = both.astype(out.dtype)
        return carry

    lax.fori_loop(0, rows // small, out_step, 0)


def half_ffn(gain, x, weights):
    (rows, full), units = (x.shape[0] // 2, x.shape[1] * 2), 2 * weights[0].shape[0]
    return pl.pallas_call(
        ffn_kernel,
        out_shape=jax.ShapeDtypeStruct(x.shape, BF16),
        in_specs=[HBM] * 8,
        out_specs=VMEM,
        scratch_shapes=[
            pltpu.VMEM(gain.shape, F32),
            pltpu.VMEM(x.shape, BF16),
            pltpu.VMEM((rows, full), BF16),
            *[pltpu.VMEM((units, full), BF16)] * 3,
            pltpu.VMEM((rows, full), F32),
            pltpu.SemaphoreType.DMA((8,)),
        ],
        cost_estimate=pl.CostEstimate(
            flops=6 * rows * full * units,
            transcendentals=rows * units,
            bytes_accessed=2 * (3 * units * full + 2 * rows * full),
        ),
        compiler_params=BIG,
    )(gain, x, *weights)


def dispatch_kernel(starts, pick, part_0, part_1, part_2, part_3, out, *whole):
    width = part_0.shape[1]
    rows, half = out.shape
    upper_row = lax.broadcasted_iota(jnp.int32, (rows, width), 0) % 8 // 4
    for k, a, b in ((0, part_0, part_3), (1, part_1, part_2)):
        is_a = upper_row == starts[k] // half
        at = pl.ds(pl.multiple_of(starts[k] % half, width), width)
        out[:, at] = jnp.where(is_a, dot(pick[...], a[...]), dot(pick[...], b[...])).astype(BF16)
    for w in whole:
        for k, part in enumerate((part_0, part_1, part_2, part_3)):
            w[:, pl.ds(pl.multiple_of(starts[k], width), width)] = part[...]


def dispatched_rows(starts, pick, parts, with_tokens):
    tokens, width = parts[0].shape
    full, rows = width * len(parts), pick.shape[0]
    shapes = [(rows, full // 2)] + [(tokens, full)] * with_tokens
    return pl.pallas_call(
        dispatch_kernel,
        out_shape=[jax.ShapeDtypeStruct(shape, BF16) for shape in shapes],
        in_specs=[SMEM] + [VMEM] * 5,
        out_specs=[VMEM] * len(shapes),
        cost_estimate=pl.CostEstimate(
            flops=2 * pick.size * full, transcendentals=0, bytes_accessed=4 * tokens * full
        ),
        compiler_params=BIG,
    )(starts, pick, *parts)


def gather_kernel(mix_hi, mix_lo, rows, base, out):
    half = rows.shape[1]
    for h in range(2):
        at = slice(h * half, (h + 1) * half)
        out[:, at] = base[:, at] + dot(mix_hi[h], rows[...]) + dot(mix_lo[h], rows[...])


def gathered(mix_hi, mix_lo, rows, base):
    return pl.pallas_call(
        gather_kernel,
        out_shape=jax.ShapeDtypeStruct(base.shape, F32),
        in_specs=[VMEM] * 4,
        out_specs=VMEM,
        cost_estimate=pl.CostEstimate(
            flops=4 * mix_hi.size * rows.shape[1], transcendentals=0, bytes_accessed=8 * base.size
        ),
        compiler_params=BIG,
    )(mix_hi, mix_lo, rows, base)


def combine_kernel(starts, mix_hi, mix_lo, rows, base, *outs, parts):
    width, half = outs[0].shape[1], rows.shape[1]
    for k, out in zip(parts, outs):
        h = starts[k] // half
        from_rows = pl.ds(pl.multiple_of(starts[k] % half, width), width)
        value = dot(mix_hi[h], rows[:, from_rows]) + dot(mix_lo[h], rows[:, from_rows])
        at = pl.ds(pl.multiple_of(starts[k], width), width)
        out[...] = (base[:, at] + value).astype(out.dtype)


def combined(starts, parts, mix_hi, mix_lo, rows, base, dtype):
    tokens, full = base.shape
    count = len(parts)
    return pl.pallas_call(
        functools.partial(combine_kernel, parts=parts),
        out_shape=[jax.ShapeDtypeStruct((tokens, full // 4), dtype)] * count,
        in_specs=[SMEM] + [VMEM] * 4,
        out_specs=[VMEM] * count,
        cost_estimate=pl.CostEstimate(
            flops=mix_hi.size * full, transcendentals=0, bytes_accessed=8 * tokens * full
        ),
        compiler_params=BIG,
    )(starts, mix_hi, mix_lo, rows, base)


def make(mesh):
    near_pairs, across_pairs, diag_pairs = pair_perms(mesh)

    def body(
        tokens,
        norm_gain,
        router_weight,
        shared_gate_w,
        expert_ids,
        w_gate,
        w_up,
        w_down,
        shared_w_gate,
        shared_w_up,
        shared_w_down,
    ):
        rows, width = tokens.shape
        peers = lax.axis_size("tp")
        slots = lax.axis_size("ep")
        full = width * peers
        share = rows // 8 // peers // CHUNKS
        me = lax.axis_index("tp")
        flip, mirror = me ^ 1, peers - 1 - me
        first_core = lax.axis_index("ep") % 2 == 0
        near = jnp.where(first_core, flip, mirror)
        across = jnp.where(first_core, mirror, flip)
        starts = jnp.stack([me, near, across, me ^ 2]).astype(jnp.int32) * width

        def to_near(value):
            return lax.ppermute(value, BOTH, near_pairs)

        def to_across(value):
            return lax.ppermute(value, BOTH, across_pairs)

        def all_parts(value):
            a, b = to_near(value), to_across(value)
            return [value, a, b, lax.ppermute(value, BOTH, diag_pairs)]

        parts = all_parts(tokens)
        own_w = (w_gate[0].T, w_up[0].T, w_down[0])
        weights = []
        for w in own_w:
            weights += [w, to_near(w)]

        experts = jnp.arange(slots, dtype=jnp.int32)
        named = jnp.any(expert_ids[:, :, None] == experts[None, None, :], axis=1)
        order = jnp.arange(rows, dtype=jnp.int32)
        earlier = (order[None, :] < order[:, None]).astype(BF16)
        before = dot(earlier, named.astype(BF16))
        key = jnp.where(named, before, -1.0).astype(BF16)
        lane = jnp.arange(slots * 2 * share, dtype=jnp.int32)
        spread = (experts[:, None] == lane[None, :] // (2 * share)).astype(BF16)
        chunk = jnp.arange(CHUNKS, dtype=jnp.int32)
        mine = ((me * CHUNKS + chunk[:, None]) * share + lane[None, :] % share).astype(F32)
        hit = dot(key, spread)[None] == mine[:, None, :]
        pick = (dot(spread, key, ((0,), (1,)))[None] == mine[:, :, None]).astype(BF16)

        (outgoing_0,) = dispatched_rows(starts, pick[0], parts, False)
        outgoing_1, whole = dispatched_rows(starts, pick[1], parts, True)
        outgoing = (outgoing_0, outgoing_1)

        values = whole.astype(F32)
        inv_rms = lax.rsqrt(jnp.mean(values * values, axis=-1, keepdims=True) + 1e-06)
        normed = (values * inv_rms * norm_gain[None, :]).astype(BF16)
        shared_gate_act = dot(normed, shared_w_gate)
        shared_up_act = dot(normed, shared_w_up)
        shared_hidden = (jax.nn.silu(shared_gate_act) * shared_up_act).astype(BF16)
        shared_part = dot(shared_hidden, shared_w_down)
        share_gate = jax.nn.sigmoid(dot(normed, shared_gate_w[:, None]))
        shared_part = lax.optimization_barrier(share_gate * shared_part)

        routers = all_parts(router_weight)
        logits = sum(
            dot(lax.dynamic_slice_in_dim(normed, starts[k], width, 1), r)
            for k, r in enumerate(routers)
        )
        probs = jax.nn.softmax(logits, axis=-1)
        probs = jnp.pad(probs, ((0, 0), (0, slots - probs.shape[1])))
        probs_hi = probs.astype(BF16)
        probs_lo = (probs - probs_hi.astype(F32)).astype(BF16)
        of_half = lane // share % 2 == jnp.arange(2, dtype=jnp.int32)[:, None]
        used = hit[:, None] & of_half[None, :, None, :]
        mix_hi = jnp.where(used, dot(probs_hi, spread)[None, None], 0.0).astype(BF16)
        mix_lo = jnp.where(used, dot(probs_lo, spread)[None, None], 0.0).astype(BF16)
        mixes = [(mix_hi[c], mix_lo[c]) for c in range(CHUNKS)]
        mixes = lax.optimization_barrier(mixes)

        gain = norm_gain[None, :]
        acc = shared_part
        for c in range(CHUNKS):
            there = outgoing[c].reshape(slots, 2 * share, full // 2)
            arrived = lax.all_to_all(there, "ep", 0, 0, tiled=True)
            arrived = arrived.reshape(outgoing[c].shape)
            arrived_far = to_across(arrived)
            sent = half_ffn(gain, arrived_far, weights)
            got = to_across(sent)
            kept = half_ffn(gain, arrived, weights)
            out = (kept.astype(F32) + got.astype(F32)).astype(BF16).reshape(there.shape)
            returned = lax.all_to_all(out, "ep", 0, 0, tiled=True)
            returned = returned.reshape(outgoing[c].shape)
            if c < CHUNKS - 1:
                acc = gathered(*mixes[c], returned, acc)
            else:
                for_diag, for_across = combined(starts, (3, 2), *mixes[c], returned, acc, BF16)
                total_near, total_me = combined(starts, (1, 0), *mixes[c], returned, acc, F32)
        came_near = to_across(for_diag)
        came_me = to_across(for_across)
        again = to_near((total_near + came_near.astype(F32)).astype(BF16))
        total_me = lax.optimization_barrier(total_me + came_me.astype(F32))
        return (total_me + again.astype(F32)).astype(BF16)

    return body


def solution(mesh):
    return jax.shard_map(
        make(mesh),
        mesh=mesh,
        in_specs=(
            P("ep", "tp"),
            P(),
            P("tp", None),
            P(),
            P("ep", None),
            P("ep", None, "tp"),
            P("ep", None, "tp"),
            P("ep", "tp", None),
            P(None, "tp"),
            P(None, "tp"),
            P("tp", None),
        ),
        out_specs=P("ep", "tp"),
        check_vma=False,
    )
```
